128 devices in a mesh: band: 64 (over y, z_lo, x, core), ga: 2 (over z_hi).
Axes of the slice: x: 4, y: 4, z: 4 (z_hi: 2, z_lo: 2; z = z_hi * 2 + z_lo), core: 2. Of those that a mesh axis runs over, the one named last changes fastest.
Arguments:
- matrix_elements: float32 [2, 16384, 12288], P(None, 'band', 'ga'), may hold values from -16 to 16
- band_index: int32 [16384], P('band'), may hold values from 0 to 1048575
- occupied: int32 [1], replicated, may hold values from 262144 to 786432
- band_weight: float32 [16384], P('band'), may hold values from 0.3 to 3
- coulomb: float32 [12288], replicated, may hold values from 0.2 to 5
Outputs:
- sigma: float32 [12288, 2, 512], P(('ga', 'band'))
The draws below stay inside these ranges and needn't reach their ends.
All inputs are finite; a program needn't handle non-finite values.
Results may differ from the reference program's by a relative error of at most 0.00018.
Values sent between devices are 32-bit elements; how exact they have to be, the bound alone decides.
A program may use at most 192 MiB of HBM per device.

```python
import math
import jax
import jax.numpy as jnp
from jax import lax

NG = 12288
COLS = 512
NB = 16384


def place_ends(drawn, rng, least, top_value):
    index_at = [jax.random.randint(jax.random.fold_in(rng, axis), (), 0, length) for axis, length in enumerate(drawn.shape)]
    widest = drawn.shape.index(max(drawn.shape))
    neighbour = index_at[:widest] + [(index_at[widest] + 1) % drawn.shape[widest]] + index_at[widest + 1:]
    return drawn.at[tuple(index_at)].set(least).at[tuple(neighbour)].set(top_value)


def strengthened(result, own_key, source, target, blocks, factor):
    owner, partner = [(jnp.arange(result.shape[axis_at]) // (result.shape[axis_at] // blocks)).reshape([-1 if axis == axis_at else 1 for axis in range(result.ndim)]) for axis_at in (source, target)]
    chosen = jax.random.permutation(own_key, blocks)[partner]
    strong = (owner == chosen) | (owner == (partner + blocks // 2) % blocks)
    return jnp.where(strong, factor * result, result)


def shard_levels(stream_key, shape, shards, smallest, top_value):
    level, own = 1.0, jax.random.fold_in(stream_key, 6)
    for axis_at, parts in shards:
        draws = jnp.exp(jax.random.uniform(jax.random.fold_in(own, axis_at), (parts,), jnp.float32, smallest / len(shards), top_value / len(shards)))
        level = level * jnp.repeat(draws, shape[axis_at] // parts).reshape([-1 if axis == axis_at else 1 for axis in range(len(shape))])
    return level


def bell_draw_with(stream_key, shape, width, bound, cuts, heavy, dtype=jnp.bfloat16):
    drawn = width * jax.random.normal(stream_key, shape, jnp.float32)
    if cuts:
        drawn = drawn * shard_levels(stream_key, shape, cuts, -0.22, 0.18)
    return jnp.clip(strengthened(drawn, jax.random.fold_in(stream_key, 3), *heavy), -bound, bound).astype(dtype)


def setup_inputs(seed: int = 0) -> dict:
    arg_keys = jax.random.split(jax.random.key(seed), 6)
    return {
        "matrix_elements": bell_draw_with(arg_keys[0], (2, NB, NG), 1.0, 16.0, ((1, 64), (2, 2)), (1, 2, 64, 4.0), jnp.float32),
        "band_index": place_ends(jax.random.randint(arg_keys[1], (NB,), 0, 1048576), jax.random.fold_in(arg_keys[1], 1), 0, 1048575).astype(jnp.int32),
        "occupied": jax.random.randint(arg_keys[2], (1,), 262144, 786433).astype(jnp.int32),
        "band_weight": jnp.clip(jnp.exp(math.log(3.0) - 2.3025851 * jax.random.uniform(arg_keys[3], (NB,), jnp.float32) ** shard_levels(arg_keys[3], (NB,), ((0, 64),), -0.2, 0.2)), 0.3, 3.0),
        "coulomb": jnp.clip(jnp.exp(jax.random.uniform(arg_keys[4], (NG,), jnp.float32, math.log(0.2), math.log(5.0))), 0.2, 5.0),
    }


def reference(matrix_elements, band_index, occupied, band_weight, coulomb):
    occ = (band_index < occupied[0]).astype(jnp.float32)
    coef = (0.5 - occ) * band_weight
    real = matrix_elements[0]
    imag = matrix_elements[1]
    left = jnp.concatenate([coef[:, None] * real, coef[:, None] * imag], 0)
    slab_re = real[:, :COLS]
    slab_im = imag[:, :COLS]
    right = jnp.concatenate([jnp.concatenate([slab_re, slab_im], 1), jnp.concatenate([slab_im, -slab_re], 1)], 0)
    factor = 1.0 / math.sqrt(NB)
    sums = lax.dot_general(left, right, (((0,), (0,)), ((), ())), precision=lax.Precision.HIGHEST, preferred_element_type=jnp.float32) * factor
    square = 2.0 - real * real - imag * imag
    defect = jnp.dot(coef, square, precision=lax.Precision.HIGHEST, preferred_element_type=jnp.float32) * factor
    weight = jnp.sqrt(coulomb[:, None] * coulomb[None, :COLS])
    part_re = weight * (sums[:, :COLS] + 0.5 * (defect[:, None] + defect[None, :COLS]))
    part_im = weight * sums[:, COLS:]
    return jnp.stack([part_re, part_im], 1)
```

```python
import functools
import math

import jax
import jax.numpy as jnp
from jax import lax
from jax.experimental import pallas as pl
from jax.experimental.pallas import tpu as pltpu
from jax.sharding import Mesh
from jax.sharding import PartitionSpec as P

COLS = 512
LANES = 128
BAND = ("band_0", "band_1", "band_2", "band_3")
GA_BAND = ("ga", "band_0", "band_1", "band_2", "band_3")
MESH = pl.DeviceIdType.MESH
RING = 4
ROUNDS = 8
F32 = jnp.float32
BF16 = jnp.bfloat16


def split(x):
    hi = x.astype(BF16)
    return hi, (x - hi.astype(F32)).astype(BF16)


def kernel(
    m_ref, bi_ref, bw_ref, occ_ref, o_ref,
    at, wst, rdef, cdef, coef, stage, slab, psend, pin,
    q, t1in, din, r1, t1in2, din2, r2, zin,
    stage_sem, slab_send, slab_sem, pair_send, pair_recv,
    t1_send, t1_recv, dr_send, dr_recv, cb_send, cb_recv,
    t1_send2, t1_recv2, dr_send2, dr_recv2, cb_send2, cb_recv2,
    z_send, z_recv,
):
    rows = o_ref.shape[0]
    half = rows // 2
    nb = m_ref.shape[1]
    group = 2 * RING * rows
    y, z, x, core, ga = (lax.axis_index(name) for name in ("band_0", "band_1", "band_2", "band_3", "ga"))
    up = lambda i: lax.rem(i + 1, RING)
    down = lambda i: lax.rem(i + RING - 1, RING)
    opposite = lambda i: lax.rem(i + 2, RING)

    barrier = pltpu.get_barrier_semaphore()
    peers = (
        {"band_3": 1 - core},
        {"band_2": up(x)},
        {"band_2": down(x)},
        {"band_0": up(y)},
        {"band_0": down(y)},
        {"band_1": 1 - z},
        {"ga": 1 - ga},
    )

    def stage_copy(i):
        zd, yy = i // RING, lax.rem(i, RING)
        start = pl.multiple_of((2 * yy + zd) * group, LANES)
        return pltpu.make_async_copy(
            m_ref.at[:, :, pl.ds(start, group)], stage.at[lax.rem(i, 2)], stage_sem.at[lax.rem(i, 2)]
        )

    def slab_local(j):
        return pltpu.make_async_copy(m_ref.at[:, :, pl.ds(j * LANES, LANES)], slab.at[j], slab_sem.at[j])

    def slab_remote(j):
        return pltpu.make_async_remote_copy(
            m_ref.at[:, :, pl.ds(j * LANES, LANES)], slab.at[j], slab_send.at[j], slab_sem.at[j],
            device_id={"ga": 1 - ga}, device_id_type=MESH,
        )

    stage_copy(jnp.int32(0)).start()
    stage_copy(jnp.int32(1)).start()

    for peer in peers:
        pl.semaphore_signal(barrier, inc=1, device_id=peer, device_id_type=MESH)
    pl.semaphore_wait(barrier, len(peers))

    @pl.when(ga == 0)
    def _():
        for j in range(COLS // LANES):
            slab_remote(j).start()
        for j in range(COLS // LANES):
            slab_local(j).start()

    c_row = (0.5 - (bi_ref[...] < occ_ref[0]).astype(F32)) * bw_ref[...]
    for i in range(nb // LANES):
        piece = c_row[:, i * LANES : (i + 1) * LANES]
        coef[pl.ds(i * LANES, LANES), :] = jnp.broadcast_to(piece, (LANES, LANES)).T

    def prep(i):
        zd, yy = i // RING, lax.rem(i, RING)
        slot = lax.rem(i, 2)
        stage_copy(i).wait()
        base = (2 * yy + zd) * group

        def column(k, carry):
            lanes = pl.ds(pl.multiple_of(k * LANES, LANES), LANES)
            here = pl.ds(pl.multiple_of(base + k * LANES, LANES), LANES)
            a = stage[slot, 0, :, lanes]
            b = stage[slot, 1, :, lanes]
            a_hi, a_lo = split(a)
            b_hi, b_lo = split(b)
            at[here, 0:nb] = a_hi.T
            at[here, nb : 2 * nb] = b_hi.T
            at[here, 2 * nb : 3 * nb] = a_lo.T
            at[here, 3 * nb : 4 * nb] = b_lo.T
            part = 0.5 * jnp.sum(coef[...] * (2.0 - a * a - b * b), axis=0, keepdims=True)
            rdef[here, :] = jnp.broadcast_to(part, (LANES, LANES)).T
            return carry

        lax.fori_loop(0, group // LANES, column, 0)

        @pl.when(i + 2 < 2 * RING)
        def _():
            stage_copy(i + 2).start()

    def weights(j):
        @pl.when(ga == 0)
        def _():
            slab_local(j).wait()

        @pl.when(ga == 1)
        def _():
            slab_remote(j).wait_recv()

        a = slab[j, 0]
        b = slab[j, 1]
        c = coef[...]
        cdef[...] = 0.5 * jnp.sum(c * (2.0 - a * a - b * b), axis=0, keepdims=True)
        a_hi, a_lo = split(c * a)
        b_hi, b_lo = split(c * b)
        for at_row, aa, bb in ((0, a_hi, b_hi), (2 * nb, a_hi, b_hi), (4 * nb, a_lo, b_lo)):
            wst[at_row : at_row + nb, 0:LANES] = aa
            wst[at_row : at_row + nb, LANES:] = bb
            wst[at_row + nb : at_row + 2 * nb, 0:LANES] = bb
            wst[at_row + nb : at_row + 2 * nb, LANES:] = -aa

    def product(yy, zd, parity):
        base = (2 * yy + zd) * group + parity * rows
        spots = [pl.ds(pl.multiple_of(base + 2 * xx * rows, 16), rows) for xx in range(RING)]
        left = jnp.concatenate([at[s, :] for s in spots], 0)
        left = jnp.concatenate([left, left[:, : 2 * nb]], 1)
        out = jnp.dot(left, wst[...], preferred_element_type=F32)
        shift = jnp.concatenate([rdef[s, :] for s in spots], 0) + cdef[...]
        return out[:, :LANES] + shift, out[:, LANES:]

    def pair_copy(r, yy):
        return pltpu.make_async_remote_copy(
            psend.at[lax.rem(r, 2), yy], pin.at[r, yy], pair_send.at[r, yy], pair_recv.at[r, yy],
            device_id={"band_3": 1 - core}, device_id_type=MESH,
        )

    first = (0, half)
    second = (half, half)

    class Stage:
        def __init__(self, held, slots, tin, landed, sems, axes):
            self.held, self.slots, self.tin, self.landed = held, slots, tin, landed
            self.sems, self.axes = sems, axes

        def chunk(self, r, k, d, part):
            return self.held.at[lax.rem(r, self.slots), k, d, :, pl.ds(*part), :]

        def send(self, which, r, k, way):
            name, me = self.axes[k]
            to = up(me) if way == 0 else down(me)
            mine, other = (first, second) if way == 0 else (second, first)
            if which == 0:
                src, dst = self.chunk(r, k, opposite(me), mine), self.tin.at[r, k, way]
            elif which == 1:
                src, dst = self.chunk(r, k, to, other), self.landed.at[r, k, way, :, pl.ds(*other), :]
            else:
                src, dst = self.chunk(r, k, to, mine), self.landed.at[r, k, way, :, pl.ds(*mine), :]
            ss, rs = self.sems[which]
            return pltpu.make_async_remote_copy(
                src, dst, ss.at[r, k, way], rs.at[r, k, way], device_id={name: to}, device_id_type=MESH
            )

        def begin(self, r):
            for which in (0, 1):
                for k in range(2):
                    for way in range(2):
                        self.send(which, r, k, way).start()

        def combine(self, r):
            slot = lax.rem(r, self.slots)
            for k in range(2):
                me = self.axes[k][1]
                for way in range(2):
                    to = up(me) if way == 0 else down(me)
                    mine = pl.ds(*(first if way == 0 else second))
                    self.send(0, r, k, way).wait_recv()
                    self.held[slot, k, to, :, mine, :] += self.tin[r, k, way]
                    self.send(2, r, k, way).start()

        def arrived(self, r):
            for which in (1, 2):
                for k in range(2):
                    for way in range(2):
                        self.send(which, r, k, way).wait_recv()

        def total(self, r, k):
            return self.held[lax.rem(r, self.slots), k, self.axes[k][1]] + self.landed[r, k, 0] + self.landed[r, k, 1]

        def sent(self, r):
            for which in range(3):
                for k in range(2):
                    for way in range(2):
                        self.send(which, r, k, way).wait_send()

    one = Stage(
        q, 4, t1in, din, ((t1_send, t1_recv), (dr_send, dr_recv), (cb_send, cb_recv)),
        (("band_2", x), ("band_0", y)),
    )
    two = Stage(
        r1, 4, t1in2, din2, ((t1_send2, t1_recv2), (dr_send2, dr_recv2), (cb_send2, cb_recv2)),
        (("band_0", y), ("band_2", x)),
    )

    def z_copy(r):
        return pltpu.make_async_remote_copy(
            r2.at[lax.rem(r, 2)], zin.at[r], z_send.at[r], z_recv.at[r],
            device_id={"band_1": 1 - z}, device_id_type=MESH,
        )

    def step(r, carry):
        @pl.when(r < 2)
        def _():
            lax.fori_loop(0, RING, lambda yy, c: (prep(r * RING + yy), c)[1], 0)

        @pl.when(r < ROUNDS)
        def _():
            j, zd = r // 2, lax.rem(r, 2)

            @pl.when(zd == 0)
            def _():
                weights(j)

            def give(yy, c):
                @pl.when(r >= 2)
                def _():
                    pair_copy(r - 2, yy).wait_send()

                re, im = product(yy, zd, 1 - core)
                for xx in range(RING):
                    psend[lax.rem(r, 2), yy, 0, xx] = re[xx * rows : (xx + 1) * rows]
                    psend[lax.rem(r, 2), yy, 1, xx] = im[xx * rows : (xx + 1) * rows]
                pair_copy(r, yy).start()
                return c

            lax.fori_loop(0, RING, give, 0)

            def keep(yy, c):
                re, im = product(yy, zd, core)
                pair_copy(r, yy).wait_recv()
                slot = lax.rem(r, 4)
                for xx in range(RING):
                    q[slot, 0, xx, yy] = re[xx * rows : (xx + 1) * rows] + pin[r, yy, 0, xx]
                    q[slot, 1, yy, xx] = im[xx * rows : (xx + 1) * rows] + pin[r, yy, 1, xx]
                return c

            lax.fori_loop(0, RING, keep, 0)
            one.begin(r)

        @pl.when((r >= ROUNDS) & (r < ROUNDS + 2))
        def _():
            lax.fori_loop(0, RING, lambda yy, c: (pair_copy(r - 2, yy).wait_send(), c)[1], 0)

        @pl.when((r >= 1) & (r < ROUNDS + 1))
        def _():
            one.combine(r - 1)

        @pl.when((r >= 2) & (r < ROUNDS + 2))
        def _():
            t = r - 2
            one.arrived(t)
            for k in range(2):
                r1[lax.rem(t, 4), k, :, 0] = one.total(t, k)
            two.begin(t)

        @pl.when((r >= 3) & (r < ROUNDS + 3))
        def _():
            two.combine(r - 3)
            one.sent(r - 3)

        @pl.when((r >= 4) & (r < ROUNDS + 4))
        def _():
            t = r - 4
            two.arrived(t)
            for k in range(2):
                r2[lax.rem(t, 2), k] = two.total(t, k)[0]

            @pl.when(lax.rem(t, 2) != z)
            def _():
                z_copy(t).start()

        @pl.when(r >= 5)
        def _():
            t = r - 5
            two.sent(t)

            @pl.when(lax.rem(t, 2) != z)
            def _():
                z_copy(t).wait_send()

            @pl.when(lax.rem(t, 2) == z)
            def _():
                z_copy(t).wait_recv()
                for k in range(2):
                    spot = pl.ds(pl.multiple_of(k * COLS + (t // 2) * LANES, LANES), LANES)
                    o_ref[:, spot] = r2[lax.rem(t, 2), k] + zin[t, k]

        return carry

    lax.fori_loop(0, ROUNDS + 5, step, 0)

    @pl.when(ga == 0)
    def _():
        for j in range(COLS // LANES):
            slab_remote(j).wait_send()


def sums_of(matrix_elements, band_index, band_weight, occupied):
    nb, ng = matrix_elements.shape[1:]
    rows = ng // (2 * RING * RING * 2)
    half = rows // 2
    group = 2 * RING * rows
    dma = pltpu.SemaphoreType.DMA
    quad = lambda: [dma((ROUNDS, 2, 2)) for _ in range(6)]
    vmem = pl.BlockSpec(memory_space=pltpu.VMEM)
    return pl.pallas_call(
        kernel,
        out_shape=jax.ShapeDtypeStruct((rows, 2 * COLS), F32),
        in_specs=[pl.BlockSpec(memory_space=pl.ANY), vmem, vmem, pl.BlockSpec(memory_space=pltpu.SMEM)],
        out_specs=vmem,
        scratch_shapes=[
            pltpu.VMEM((ng, 4 * nb), BF16),
            pltpu.VMEM((6 * nb, 2 * LANES), BF16),
            pltpu.VMEM((ng, LANES), F32),
            pltpu.VMEM((1, LANES), F32),
            pltpu.VMEM((nb, LANES), F32),
            pltpu.VMEM((2, 2, nb, group), F32),
            pltpu.VMEM((COLS // LANES, 2, nb, LANES), F32),
            pltpu.VMEM((2, RING, 2, RING, rows, LANES), F32),
            pltpu.VMEM((ROUNDS, RING, 2, RING, rows, LANES), F32),
            pltpu.VMEM((4, 2, RING, RING, rows, LANES), F32),
            pltpu.VMEM((ROUNDS, 2, 2, RING, half, LANES), F32),
            pltpu.VMEM((ROUNDS, 2, 2, RING, rows, LANES), F32),
            pltpu.VMEM((4, 2, RING, 1, rows, LANES), F32),
            pltpu.VMEM((ROUNDS, 2, 2, 1, half, LANES), F32),
            pltpu.VMEM((ROUNDS, 2, 2, 1, rows, LANES), F32),
            pltpu.VMEM((2, 2, rows, LANES), F32),
            pltpu.VMEM((ROUNDS, 2, rows, LANES), F32),
            dma((2,)), dma((COLS // LANES,)), dma((COLS // LANES,)),
            dma((ROUNDS, RING)), dma((ROUNDS, RING)),
            *quad(), *quad(),
            dma((ROUNDS,)), dma((ROUNDS,)),
        ],
        compiler_params=pltpu.CompilerParams(
            collective_id=0, has_side_effects=True, vmem_limit_bytes=67043328
        ),
        name="remainder_sums",
    )(matrix_elements, band_index.reshape(1, nb), band_weight.reshape(1, nb), occupied)


def body(matrix_elements, band_index, occupied, band_weight, coulomb):
    bands_dev, half = matrix_elements.shape[1:]
    n_band = lax.axis_size(BAND)
    rows_dev = half // n_band
    factor = 1.0 / math.sqrt(bands_dev * n_band)
    sums = sums_of(matrix_elements, band_index, band_weight, occupied)
    start = lax.axis_index("ga") * half + lax.axis_index(BAND) * rows_dev
    row_coul = lax.dynamic_slice_in_dim(coulomb, start, rows_dev, 0)
    weight = jnp.sqrt(row_coul[:, None] * coulomb[None, :COLS])
    return sums.reshape(rows_dev, 2, COLS) * factor * weight[:, None, :]


def solution(mesh):
    finer = Mesh(
        mesh.devices.reshape(4, 2, 4, 2, mesh.shape["ga"]),
        ("band_0", "band_1", "band_2", "band_3", "ga"),
    )
    in_specs = (P(None, BAND, "ga"), P(BAND), P(), P(BAND), P())
    out_specs = P(GA_BAND, None, None)
    return jax.shard_map(body, mesh=finer, in_specs=in_specs, out_specs=out_specs, check_vma=False)
```

```python
import functools
import math

import jax
import jax.numpy as jnp
from jax import lax
from jax.experimental import pallas as pl
from jax.experimental.pallas import tpu as pltpu
from jax.sharding import Mesh
from jax.sharding import PartitionSpec as P

COLS = 512
LANES = 128
BAND = ("band_0", "band_1", "band_2", "band_3")
GA_BAND = ("ga", "band_0", "band_1", "band_2", "band_3")
MESH = pl.DeviceIdType.MESH
Z_ORDER = (2, 3, 1, 0)
RING = 4
PARTS = 2
ROUNDS = 4 * PARTS
LAGS = (1, 2, 3, 4, 5)
SLOTS = 4
STAGES = 4
F32 = jnp.float32
BF16 = jnp.bfloat16


def split(x):
    hi = x.astype(BF16)
    return hi, (x - hi.astype(F32)).astype(BF16)


def kernel(
    m_ref, bi_ref, bw_ref, coul_ref, occ_ref, o_ref,
    at, wst, rdef, cdef, coef, rowc, stage, slab, psend, pin,
    q, t1in, din, r1, zin, rz, t1in2, din2,
    stage_sem, slab_copy, slab_send, slab_recv, pair_send, pair_recv,
    t1_send, t1_recv, in_send, in_recv, t1_send2, t1_recv2, in_send2, in_recv2,
    z_send, z_recv,
):
    rows = o_ref.shape[0]
    part = rows // PARTS
    nb = m_ref.shape[1]
    ng = m_ref.shape[2]
    n_chunks = COLS // LANES
    scale = 1.0 / math.sqrt(nb * 2 * RING * RING * 2)
    group = 2 * RING * rows
    y, z, x, core, ga = (lax.axis_index(name) for name in ("band_0", "band_1", "band_2", "band_3", "ga"))
    up = lambda i: lax.rem(i + 1, RING)
    down = lambda i: lax.rem(i + RING - 1, RING)
    opposite = lambda i: lax.rem(i + 2, RING)

    barrier = pltpu.get_barrier_semaphore()
    peers = (
        {"ga": 1 - ga},
        {"band_2": up(x)},
        {"band_2": down(x)},
        {"band_0": up(y)},
        {"band_0": down(y)},
        {"band_1": 1 - z},
        {"band_3": 1 - core},
    )
    for peer in peers:
        pl.semaphore_signal(barrier, inc=1, device_id=peer, device_id_type=MESH)

    def stage_copy(i):
        start = pl.multiple_of(i * group, LANES)
        return pltpu.make_async_copy(
            m_ref.at[:, :, pl.ds(start, group)], stage.at[lax.rem(i, STAGES)], stage_sem.at[lax.rem(i, STAGES)]
        )

    def size_of(ref, send_sem, recv_sem):
        return pltpu.make_async_remote_copy(
            ref, ref, send_sem, recv_sem, device_id={"band_3": 1 - core}, device_id_type=MESH
        )

    def slab_local(j):
        return pltpu.make_async_copy(m_ref.at[:, :, pl.ds(j * LANES, LANES)], slab.at[j], slab_copy.at[0])

    def slab_remote(j):
        return pltpu.make_async_remote_copy(
            slab.at[j], slab.at[j], slab_send.at[0], slab_recv.at[j],
            device_id={"ga": 1 - ga}, device_id_type=MESH,
        )

    @pl.when(ga == 0)
    def _():
        for j in range(n_chunks):
            slab_local(j).start()

    for i in range(STAGES):
        stage_copy(jnp.int32(i)).start()

    c_row = (0.5 - (bi_ref[...] < occ_ref[0]).astype(F32)) * bw_ref[...]
    for i in range(nb // LANES):
        piece = c_row[:, i * LANES : (i + 1) * LANES]
        coef[pl.ds(i * LANES, LANES), :] = jnp.broadcast_to(piece, (LANES, LANES)).T

    total_g = coul_ref.shape[1]
    row_start = ga * ng + (((y * 2 + z) * RING + x) * 2 + core) * rows
    block = (row_start // LANES) * LANES
    after = lax.rem(block + LANES, total_g)
    window = jnp.concatenate(
        [coul_ref[:, pl.ds(pl.multiple_of(b, LANES), LANES)] for b in (block, after)], 1
    )
    window = pltpu.roll(jnp.broadcast_to(window, (8, 2 * LANES)), lax.rem(2 * LANES - (row_start - block), 2 * LANES), 1)
    rowc[...] = jnp.broadcast_to(window[:1, :LANES], (LANES, LANES)).T

    def prep(i, carry):
        slot = lax.rem(i, STAGES)
        stage_copy(i).wait()

        def column(k, carry):
            lanes = pl.ds(pl.multiple_of(k * LANES, LANES), LANES)
            here = pl.ds(pl.multiple_of(i * group + k * LANES, LANES), LANES)
            a = stage[slot, 0, :, lanes]
            b = stage[slot, 1, :, lanes]
            a_hi, a_lo = split(a)
            b_hi, b_lo = split(b)
            at[here, 0:nb] = a_hi.T
            at[here, nb : 2 * nb] = b_hi.T
            at[here, 2 * nb : 3 * nb] = a_lo.T
            at[here, 3 * nb : 4 * nb] = b_lo.T
            share = 0.5 * jnp.sum(coef[...] * (2.0 - a * a - b * b), axis=0, keepdims=True)
            rdef[here, :] = jnp.broadcast_to(share, (LANES, LANES)).T
            return carry

        lax.fori_loop(0, group // LANES, column, 0)

        @pl.when(i + STAGES < 2 * RING)
        def _():
            stage_copy(i + STAGES).start()

        return carry

    prep(jnp.int32(0), 0)

    @pl.when(ga == 0)
    def _():
        pltpu.make_async_copy(slab, slab, slab_copy.at[0]).wait()

    pl.semaphore_wait(barrier, len(peers))

    @pl.when(ga == 0)
    def _():
        for j in range(n_chunks):
            slab_remote(j).start()

    lax.fori_loop(1, 2 * RING, prep, 0)

    def weights(j):
        @pl.when(ga == 1)
        def _():
            slab_remote(j).wait_recv()

        w = lax.rem(j, 2)
        a = slab[j, 0]
        b = slab[j, 1]
        c = coef[...]
        cdef[w] = 0.5 * jnp.sum(c * (2.0 - a * a - b * b), axis=0, keepdims=True)
        a_hi, a_lo = split(c * a)
        b_hi, b_lo = split(c * b)
        for at_row, aa, bb in ((0, a_hi, b_hi), (2 * nb, a_hi, b_hi), (4 * nb, a_lo, b_lo)):
            wst[w, at_row : at_row + nb, 0:LANES] = aa
            wst[w, at_row : at_row + nb, LANES:] = bb
            wst[w, at_row + nb : at_row + 2 * nb, 0:LANES] = bb
            wst[w, at_row + nb : at_row + 2 * nb, LANES:] = -aa

    pieces = [(y2, zd, xx) for y2 in range(2) for zd in range(2) for xx in range(RING)]

    def product(r, g, parity):
        w = lax.rem(r // PARTS, 2)
        base = g * (4 * group) + parity * rows + lax.rem(r, PARTS) * part
        spots = [
            pl.ds(pl.multiple_of(base + (2 * y2 + zd) * group + 2 * xx * rows, 16), part)
            for y2, zd, xx in pieces
        ]
        left = jnp.concatenate([at[s, :] for s in spots], 0)
        left = jnp.concatenate([left, left[:, : 2 * nb]], 1)
        out = jnp.dot(left, wst[w], preferred_element_type=F32)
        shift = jnp.concatenate([rdef[s, :] for s in spots], 0) + cdef[w]
        return out[:, :LANES] + shift, out[:, LANES:]

    def pair_copy(r, g):
        return pltpu.make_async_remote_copy(
            psend.at[lax.rem(r, 2), g], pin.at[r, g], pair_send.at[lax.rem(r, 2), g], pair_recv.at[r, g],
            device_id={"band_3": 1 - core}, device_id_type=MESH,
        )

    def give(r):
        @pl.when(lax.rem(r, PARTS) == 0)
        def _():
            weights(r // PARTS)

        def one_pair(g, carry):
            @pl.when(r >= 2)
            def _():
                pair_copy(r - 2, g).wait_send()

            re, im = product(r, g, 1 - core)
            for n, (y2, zd, xx) in enumerate(pieces):
                psend[lax.rem(r, 2), g, 0, zd, y2, xx] = re[n * part : (n + 1) * part]
                psend[lax.rem(r, 2), g, 1, zd, y2, xx] = im[n * part : (n + 1) * part]
            pair_copy(r, g).start()
            return carry

        lax.fori_loop(0, 2, one_pair, 0)

    def keep(r):
        slot = lax.rem(r, SLOTS)

        def one_pair(g, carry):
            re, im = product(r, g, core)
            pair_copy(r, g).wait_recv()
            for n, (y2, zd, xx) in enumerate(pieces):
                q[slot, 0, xx, zd, 2 * g + y2] = re[n * part : (n + 1) * part] + pin[r, g, 0, zd, y2, xx]
                q[slot, 1, 2 * g + y2, zd, xx] = im[n * part : (n + 1) * part] + pin[r, g, 1, zd, y2, xx]
            return carry

        lax.fori_loop(0, 2, one_pair, 0)

    class Stage:
        def __init__(self, held, tin, landed, cut, sems, axes):
            self.held, self.tin, self.landed = held, tin, landed
            self.cut, self.sems, self.axes = cut, sems, axes

        def send(self, which, r, k, way):
            name, me = self.axes[k]
            to = up(me) if way == 0 else down(me)
            here = self.cut(way if which != 1 else 1 - way)
            chunk = (lax.rem(r, SLOTS), k, opposite(me) if which == 0 else to)
            src = self.held.at[chunk + here]
            dst = self.tin.at[r, k, way] if which == 0 else self.landed.at[(r, k, way) + here]
            ss, rs = self.sems[min(which, 1)]
            return pltpu.make_async_remote_copy(
                src, dst, ss.at[lax.rem(r, SLOTS)], rs.at[r], device_id={name: to}, device_id_type=MESH
            )

        def whole(self, which, r):
            ref = (self.tin if which == 0 else self.landed).at[r]
            ss, rs = self.sems[which]
            return size_of(ref, ss.at[lax.rem(r, SLOTS)], rs.at[r])

        def begin(self, r, which, k):
            for way in range(2):
                self.send(which, r, k, way).start()

        def combine(self, r):
            self.whole(0, r).wait_recv()
            for k in range(2):
                me = self.axes[k][1]
                for way in range(2):
                    to = up(me) if way == 0 else down(me)
                    here = (lax.rem(r, SLOTS), k, to) + self.cut(way)
                    self.held[here] += self.tin[r, k, way]
                    self.send(2, r, k, way).start()

        def arrived(self, r):
            self.whole(1, r).wait_recv()

        def total(self, r, k):
            return self.held[lax.rem(r, SLOTS), k, self.axes[k][1]] + self.landed[r, k, 0] + self.landed[r, k, 1]

        def sent(self, r):
            self.whole(0, r).wait_send()
            self.whole(1, r).wait_send()

    along_x, along_y = ("band_2", x), ("band_0", y)
    one = Stage(
        q, t1in, din, lambda h: (h,),
        ((t1_send, t1_recv), (in_send, in_recv)), (along_x, along_y),
    )
    two = Stage(
        rz, t1in2, din2, lambda h: (pl.ds(h * (part // 2), part // 2),),
        ((t1_send2, t1_recv2), (in_send2, in_recv2)), (along_y, along_x),
    )

    def z_copy(r, k, m):
        e = lax.rem(two.axes[k][1] + Z_ORDER[m], RING)
        return pltpu.make_async_remote_copy(
            r1.at[lax.rem(r, SLOTS), k, 1 - z, e], zin.at[r, k, e],
            z_send.at[lax.rem(r, SLOTS), min(m, 1)], z_recv.at[r, min(m, 1)],
            device_id={"band_1": 1 - z}, device_id_type=MESH,
        )

    def z_whole(r, n):
        ref = zin.at[r, :, pl.ds(n, 1 + 2 * n)]
        return size_of(ref, z_send.at[lax.rem(r, SLOTS), n], z_recv.at[r, n])

    def to_other_z(t):
        one.arrived(t)
        for k in range(2):
            r1[lax.rem(t, SLOTS), k] = one.total(t, k)
        for m in range(RING):
            for k in range(2):
                z_copy(t, k, m).start()

    def from_other_z(t):
        slot = lax.rem(t, SLOTS)
        for which, ms in ((0, (0,)), (1, (1, 2, 3))):
            z_whole(t, which).wait_recv()
            for k in range(2):
                for m in ms:
                    e = lax.rem(two.axes[k][1] + Z_ORDER[m], RING)
                    rz[slot, k, e] = r1[slot, k, z, e] + zin[t, k, e]
                two.begin(t, which, k)
        one.sent(t)

    def second_combine(t):
        two.combine(t)
        for n in range(2):
            z_whole(t, n).wait_send()

    def finish(t):
        down_to = pl.ds(pl.multiple_of(lax.rem(t, PARTS) * part, 8), part)
        lanes = pl.multiple_of((t // PARTS) * LANES, LANES)
        weight = jnp.sqrt(rowc[down_to, :] * coul_ref[:, pl.ds(lanes, LANES)]) * scale
        two.arrived(t)
        for k in range(2):
            o_ref[down_to, k, pl.ds(lanes, LANES)] = two.total(t, k) * weight
        two.sent(t)

    give(jnp.int32(0))

    def step(r, carry):
        @pl.when(r + 1 < ROUNDS)
        def _():
            give(r + 1)

        @pl.when(r < ROUNDS)
        def _():
            keep(r)
            for which in (0, 1):
                for k in range(2):
                    one.begin(r, which, k)

        def late(lag, stage_work):
            @pl.when((r >= lag) & (r < ROUNDS + lag))
            def _():
                stage_work(r - lag)

        for lag, stage_work in zip(LAGS, (one.combine, to_other_z, from_other_z, second_combine, finish)):
            late(lag, stage_work)

        return carry

    lax.fori_loop(0, ROUNDS + LAGS[-1], step, 0)

    for g in range(2):
        pair_copy(ROUNDS - 2, g).wait_send()
        pair_copy(ROUNDS - 1, g).wait_send()

    @pl.when(ga == 0)
    def _():
        size_of(slab, slab_send.at[0], slab_recv.at[0]).wait_send()


def sums_of(matrix_elements, band_index, band_weight, coulomb, occupied):
    nb, ng = matrix_elements.shape[1:]
    rows = ng // (2 * RING * RING * 2)
    part = rows // PARTS
    group = 2 * RING * rows
    n_chunks = COLS // LANES
    dma = pltpu.SemaphoreType.DMA
    ring = lambda: [dma((n,)) for n in (SLOTS, ROUNDS, SLOTS, ROUNDS)]
    vmem = pl.BlockSpec(memory_space=pltpu.VMEM)
    return pl.pallas_call(
        kernel,
        out_shape=jax.ShapeDtypeStruct((rows, 2, COLS), F32),
        in_specs=[pl.BlockSpec(memory_space=pl.ANY), vmem, vmem, vmem, pl.BlockSpec(memory_space=pltpu.SMEM)],
        out_specs=vmem,
        scratch_shapes=[
            pltpu.VMEM((ng, 4 * nb), BF16),
            pltpu.VMEM((2, 6 * nb, 2 * LANES), BF16),
            pltpu.VMEM((ng, LANES), F32),
            pltpu.VMEM((2, 1, LANES), F32),
            pltpu.VMEM((nb, LANES), F32),
            pltpu.VMEM((LANES, LANES), F32),
            pltpu.VMEM((STAGES, 2, nb, group), F32),
            pltpu.VMEM((n_chunks, 2, nb, LANES), F32),
            pltpu.VMEM((2, 2, 2, 2, 2, RING, part, LANES), F32),
            pltpu.VMEM((ROUNDS, 2, 2, 2, 2, RING, part, LANES), F32),
            pltpu.VMEM((SLOTS, 2, RING, 2, RING, part, LANES), F32),
            pltpu.VMEM((ROUNDS, 2, 2, RING, part, LANES), F32),
            pltpu.VMEM((ROUNDS, 2, 2, 2, RING, part, LANES), F32),
            pltpu.VMEM((SLOTS, 2, 2, RING, part, LANES), F32),
            pltpu.VMEM((ROUNDS, 2, RING, part, LANES), F32),
            pltpu.VMEM((SLOTS, 2, RING, part, LANES), F32),
            pltpu.VMEM((ROUNDS, 2, 2, part // 2, LANES), F32),
            pltpu.VMEM((ROUNDS, 2, 2, part, LANES), F32),
            dma((STAGES,)), dma((1,)), dma((1,)), dma((n_chunks,)),
            dma((2, 2)), dma((ROUNDS, 2)),
            *ring(), *ring(),
            dma((SLOTS, 2)), dma((ROUNDS, 2)),
        ],
        compiler_params=pltpu.CompilerParams(
            collective_id=0, has_side_effects=True, vmem_limit_bytes=67043328
        ),
        name="remainder_sums",
    )(
        matrix_elements, band_index.reshape(1, nb), band_weight.reshape(1, nb),
        coulomb.reshape(1, -1), occupied,
    )


def body(matrix_elements, band_index, occupied, band_weight, coulomb):
    return sums_of(matrix_elements, band_index, band_weight, coulomb, occupied)


def solution(mesh):
    finer = Mesh(
        mesh.devices.reshape(4, 2, 4, 2, mesh.shape["ga"]),
        ("band_0", "band_1", "band_2", "band_3", "ga"),
    )
    in_specs = (P(None, BAND, "ga"), P(BAND), P(), P(BAND), P())
    out_specs = P(GA_BAND, None, None)
    return jax.shard_map(body, mesh=finer, in_specs=in_specs, out_specs=out_specs, check_vma=False)
```

```python
import functools
import math

import jax
import jax.numpy as jnp
from jax import lax
from jax.experimental import pallas as pl
from jax.experimental.pallas import tpu as pltpu
from jax.sharding import Mesh
from jax.sharding import PartitionSpec as P

COLS = 512
LANES = 128
BAND = ("band_0", "band_1", "band_2", "band_3")
GA_BAND = ("ga", "band_0", "band_1", "band_2", "band_3")
MESH = pl.DeviceIdType.MESH
Z_ORDER = (2, 3, 1, 0)
Z_GROUP = (0, 1, 1, 2)
RING = 4
PARTS = 2
ROUNDS = 4 * PARTS
LAGS = (2, 3, 4, 5)
SLOTS = 4
STAGES = 4
F32 = jnp.float32
BF16 = jnp.bfloat16


def split(x):
    hi = x.astype(BF16)
    return hi, (x - hi.astype(F32)).astype(BF16)


def kernel(
    m_ref, bi_in, bw_in, coul_in, occ_ref, o_ref,
    bi_ref, bw_ref, coul_ref, at, wst, rdef, cdef, coef, rowc, stage, slab, psend, pin,
    q, t1in, din, r1, zin, rz, t1in2, din2,
    stage_sem, slab_copy, slab_send, slab_recv, pair_send, pair_recv,
    t1_send, t1_recv, in_send, in_recv, t1_send2, t1_recv2, in_send2, in_recv2,
    z_send, z_recv, small_sem,
):
    rows = o_ref.shape[0]
    part = rows // PARTS
    nb = m_ref.shape[1]
    ng = m_ref.shape[2]
    n_chunks = COLS // LANES
    scale = 1.0 / math.sqrt(nb * 2 * RING * RING * 2)
    group = 2 * RING * rows
    y, z, x, core, ga = (lax.axis_index(name) for name in ("band_0", "band_1", "band_2", "band_3", "ga"))
    up = lambda i: lax.rem(i + 1, RING)
    down = lambda i: lax.rem(i + RING - 1, RING)
    opposite = lambda i: lax.rem(i + 2, RING)

    barrier = pltpu.get_barrier_semaphore()
    peers = (
        {"ga": 1 - ga},
        {"band_2": up(x)},
        {"band_2": down(x)},
        {"band_0": up(y)},
        {"band_0": down(y)},
        {"band_1": 1 - z},
        {"band_3": 1 - core},
    )
    for peer in peers:
        pl.semaphore_signal(barrier, inc=1, device_id=peer, device_id_type=MESH)

    def stage_copy(i):
        start = pl.multiple_of(i * group, LANES)
        return pltpu.make_async_copy(
            m_ref.at[:, :, pl.ds(start, group)], stage.at[lax.rem(i, STAGES)], stage_sem.at[lax.rem(i, STAGES)]
        )

    def size_of(ref, send_sem, recv_sem):
        return pltpu.make_async_remote_copy(
            ref, ref, send_sem, recv_sem, device_id={"band_3": 1 - core}, device_id_type=MESH
        )

    def slab_local(j):
        return pltpu.make_async_copy(m_ref.at[:, :, pl.ds(j * LANES, LANES)], slab.at[j], slab_copy.at[0])

    def slab_remote(j):
        return pltpu.make_async_remote_copy(
            slab.at[j], slab.at[j], slab_send.at[0], slab_recv.at[j],
            device_id={"ga": 1 - ga}, device_id_type=MESH,
        )

    @pl.when(ga == 0)
    def _():
        for j in range(n_chunks):
            slab_local(j).start()

    small = [
        pltpu.make_async_copy(src, dst, small_sem.at[n])
        for n, (src, dst) in enumerate(((bi_in, bi_ref), (bw_in, bw_ref), (coul_in, coul_ref)))
    ]
    stage_copy(jnp.int32(0)).start()
    for copy in small:
        copy.start()
    for i in range(1, STAGES):
        stage_copy(jnp.int32(i)).start()
    for copy in small:
        copy.wait()

    c_row = (0.5 - (bi_ref[...] < occ_ref[0]).astype(F32)) * bw_ref[...]
    for i in range(nb // LANES):
        piece = c_row[:, i * LANES : (i + 1) * LANES]
        coef[pl.ds(i * LANES, LANES), :] = jnp.broadcast_to(piece, (LANES, LANES)).T

    @pl.when(ga == 0)
    def _():
        pltpu.make_async_copy(slab, slab, slab_copy.at[0]).wait()

    pl.semaphore_wait(barrier, len(peers))

    @pl.when(ga == 0)
    def _():
        for j in range(n_chunks):
            slab_remote(j).start()

    total_g = coul_ref.shape[1]
    row_start = ga * ng + (((y * 2 + z) * RING + x) * 2 + core) * rows
    block = (row_start // LANES) * LANES
    after = lax.rem(block + LANES, total_g)
    window = jnp.concatenate(
        [coul_ref[:, pl.ds(pl.multiple_of(b, LANES), LANES)] for b in (block, after)], 1
    )
    window = pltpu.roll(jnp.broadcast_to(window, (8, 2 * LANES)), lax.rem(2 * LANES - (row_start - block), 2 * LANES), 1)
    rowc[...] = jnp.broadcast_to(window[:1, :LANES], (LANES, LANES)).T

    def prep(i, carry):
        slot = lax.rem(i, STAGES)
        stage_copy(i).wait()

        def column(k, carry):
            lanes = pl.ds(pl.multiple_of(k * LANES, LANES), LANES)
            here = pl.ds(pl.multiple_of(i * group + k * LANES, LANES), LANES)
            a = stage[slot, 0, :, lanes]
            b = stage[slot, 1, :, lanes]
            a_hi, a_lo = split(a)
            b_hi, b_lo = split(b)
            at[here, 0:nb] = a_hi.T
            at[here, nb : 2 * nb] = b_hi.T
            at[here, 2 * nb : 3 * nb] = a_lo.T
            at[here, 3 * nb : 4 * nb] = b_lo.T
            share = 0.5 * jnp.sum(coef[...] * (2.0 - a * a - b * b), axis=0, keepdims=True)
            rdef[here, :] = jnp.broadcast_to(share, (LANES, LANES)).T
            return carry

        lax.fori_loop(0, group // LANES, column, 0)

        @pl.when(i + STAGES < 2 * RING)
        def _():
            stage_copy(i + STAGES).start()

        return carry

    lax.fori_loop(0, RING + RING * ga, prep, 0)

    def weights(j):
        @pl.when(ga == 1)
        def _():
            slab_remote(j).wait_recv()

        w = lax.rem(j, 2)
        a = slab[j, 0]
        b = slab[j, 1]
        c = coef[...]
        cdef[w] = 0.5 * jnp.sum(c * (2.0 - a * a - b * b), axis=0, keepdims=True)
        a_hi, a_lo = split(c * a)
        b_hi, b_lo = split(c * b)
        for at_row, aa, bb in ((0, a_hi, b_hi), (2 * nb, a_hi, b_hi), (4 * nb, a_lo, b_lo)):
            wst[w, at_row : at_row + nb, 0:LANES] = aa
            wst[w, at_row : at_row + nb, LANES:] = bb
            wst[w, at_row + nb : at_row + 2 * nb, 0:LANES] = bb
            wst[w, at_row + nb : at_row + 2 * nb, LANES:] = -aa

    pieces = [(y2, zd, xx) for y2 in range(2) for zd in range(2) for xx in range(RING)]

    def product(r, g, parity):
        w = lax.rem(r // PARTS, 2)
        base = g * (4 * group) + parity * rows + lax.rem(r, PARTS) * part
        spots = [
            pl.ds(pl.multiple_of(base + (2 * y2 + zd) * group + 2 * xx * rows, 16), part)
            for y2, zd, xx in pieces
        ]
        left = jnp.concatenate([at[s, :] for s in spots], 0)
        left = jnp.concatenate([left, left[:, : 2 * nb]], 1)
        out = jnp.dot(left, wst[w], preferred_element_type=F32)
        shift = jnp.concatenate([rdef[s, :] for s in spots], 0) + cdef[w]
        return out[:, :LANES] + shift, out[:, LANES:]

    def pair_copy(r, g):
        return pltpu.make_async_remote_copy(
            psend.at[lax.rem(r, 2), g], pin.at[r, g], pair_send.at[lax.rem(r, 2), g], pair_recv.at[r, g],
            device_id={"band_3": 1 - core}, device_id_type=MESH,
        )

    def give(r):
        @pl.when(lax.rem(r, PARTS) == 0)
        def _():
            weights(r // PARTS)

        def one_pair(g, carry):
            @pl.when((r == 0) & (g == 1))
            def _():
                lax.fori_loop(RING + RING * ga, 2 * RING, prep, 0)

            @pl.when(r >= 2)
            def _():
                pair_copy(r - 2, g).wait_send()

            re, im = product(r, g, 1 - core)
            for n, (y2, zd, xx) in enumerate(pieces):
                psend[lax.rem(r, 2), g, 0, zd, y2, xx] = re[n * part : (n + 1) * part]
                psend[lax.rem(r, 2), g, 1, zd, y2, xx] = im[n * part : (n + 1) * part]
            pair_copy(r, g).start()
            return carry

        lax.fori_loop(0, 2, one_pair, 0)

    def keep(r):
        slot = lax.rem(r, SLOTS)

        def one_pair(g, carry):
            re, im = product(r, g, core)
            pair_copy(r, g).wait_recv()
            for n, (y2, zd, xx) in enumerate(pieces):
                q[slot, 0, xx, zd, 2 * g + y2] = re[n * part : (n + 1) * part] + pin[r, g, 0, zd, y2, xx]
                q[slot, 1, 2 * g + y2, zd, xx] = im[n * part : (n + 1) * part] + pin[r, g, 1, zd, y2, xx]
            return carry

        lax.fori_loop(0, 2, one_pair, 0)

    class Stage:
        def __init__(self, held, tin, landed, cut, sems, axes):
            self.held, self.tin, self.landed = held, tin, landed
            self.cut, self.sems, self.axes = cut, sems, axes

        def send(self, which, r, k, way):
            name, me = self.axes[k]
            to = up(me) if way == 0 else down(me)
            here = self.cut(way if which != 1 else 1 - way)
            chunk = (lax.rem(r, SLOTS), k, opposite(me) if which == 0 else to)
            src = self.held.at[chunk + here]
            dst = self.tin.at[r, k, way] if which == 0 else self.landed.at[(r, k, way) + here]
            ss, rs = self.sems[min(which, 1)]
            return pltpu.make_async_remote_copy(
                src, dst, ss.at[lax.rem(r, SLOTS)], rs.at[r], device_id={name: to}, device_id_type=MESH
            )

        def whole(self, which, r):
            ref = (self.tin if which == 0 else self.landed).at[r]
            ss, rs = self.sems[which]
            return size_of(ref, ss.at[lax.rem(r, SLOTS)], rs.at[r])

        def begin(self, r, which, k):
            for way in range(2):
                self.send(which, r, k, way).start()

        def combine(self, r):
            self.whole(0, r).wait_recv()
            for k in range(2):
                me = self.axes[k][1]
                for way in range(2):
                    to = up(me) if way == 0 else down(me)
                    here = (lax.rem(r, SLOTS), k, to) + self.cut(way)
                    self.held[here] += self.tin[r, k, way]
                    self.send(2, r, k, way).start()

        def arrived(self, r):
            self.whole(1, r).wait_recv()

        def total(self, r, k):
            return self.held[lax.rem(r, SLOTS), k, self.axes[k][1]] + self.landed[r, k, 0] + self.landed[r, k, 1]

        def sent(self, r):
            self.whole(0, r).wait_send()
            self.whole(1, r).wait_send()

    along_x, along_y = ("band_2", x), ("band_0", y)
    one = Stage(
        q, t1in, din, lambda h: (h,),
        ((t1_send, t1_recv), (in_send, in_recv)), (along_x, along_y),
    )
    two = Stage(
        rz, t1in2, din2, lambda h: (pl.ds(h * (part // 2), part // 2),),
        ((t1_send2, t1_recv2), (in_send2, in_recv2)), (along_y, along_x),
    )

    def z_copy(r, k, m):
        e = lax.rem(two.axes[k][1] + Z_ORDER[m], RING)
        return pltpu.make_async_remote_copy(
            r1.at[lax.rem(r, SLOTS), k, 1 - z, e], zin.at[r, k, e],
            z_send.at[lax.rem(r, SLOTS), Z_GROUP[m]], z_recv.at[r, Z_GROUP[m]],
            device_id={"band_1": 1 - z}, device_id_type=MESH,
        )

    def z_whole(r, n):
        ref = zin.at[r, :, pl.ds(n, Z_GROUP.count(n))]
        return size_of(ref, z_send.at[lax.rem(r, SLOTS), n], z_recv.at[r, n])

    def to_other_z(t):
        one.arrived(t)
        for k in range(2):
            r1[lax.rem(t, SLOTS), k] = one.total(t, k)
        for m in range(RING):
            for k in range(2):
                z_copy(t, k, m).start()

    def from_other_z(t):
        slot = lax.rem(t, SLOTS)
        for which in range(2):
            z_whole(t, which).wait_recv()
            for k in range(2):
                for m in (m for m in range(RING) if Z_GROUP[m] == which):
                    e = lax.rem(two.axes[k][1] + Z_ORDER[m], RING)
                    rz[slot, k, e] = r1[slot, k, z, e] + zin[t, k, e]
                two.begin(t, which, k)
        one.sent(t)

    def second_combine(t):
        two.combine(t)
        for n in range(3):
            z_whole(t, n).wait_send()

    def finish(t):
        down_to = pl.ds(pl.multiple_of(lax.rem(t, PARTS) * part, 8), part)
        lanes = pl.multiple_of((t // PARTS) * LANES, LANES)
        weight = jnp.sqrt(rowc[down_to, :] * coul_ref[:, pl.ds(lanes, LANES)]) * scale
        z_whole(t, 2).wait_recv()
        two.arrived(t)
        slot = lax.rem(t, SLOTS)
        for k in range(2):
            me = two.axes[k][1]
            rz[slot, k, me] = r1[slot, k, z, me] + zin[t, k, me]
            o_ref[down_to, k, pl.ds(lanes, LANES)] = two.total(t, k) * weight
        two.sent(t)

    def step(r, carry):
        @pl.when((r >= 0) & (r < ROUNDS))
        def _():
            keep(r)
            for k in range(2):
                one.begin(r, 0, k)

        @pl.when((r >= 1) & (r < ROUNDS + 1))
        def _():
            one.combine(r - 1)

        @pl.when((r >= 0) & (r < ROUNDS))
        def _():
            for k in range(2):
                one.begin(r, 1, k)

        @pl.when(r + 1 < ROUNDS)
        def _():
            give(r + 1)

        def late(lag, stage_work):
            @pl.when((r >= lag) & (r < ROUNDS + lag))
            def _():
                stage_work(r - lag)

        for lag, stage_work in zip(LAGS, (to_other_z, from_other_z, second_combine, finish)):
            late(lag, stage_work)

        return carry

    lax.fori_loop(-1, ROUNDS + LAGS[-1], step, 0)

    for g in range(2):
        pair_copy(ROUNDS - 2, g).wait_send()
        pair_copy(ROUNDS - 1, g).wait_send()

    @pl.when(ga == 0)
    def _():
        size_of(slab, slab_send.at[0], slab_recv.at[0]).wait_send()


def sums_of(matrix_elements, band_index, band_weight, coulomb, occupied):
    nb, ng = matrix_elements.shape[1:]
    rows = ng // (2 * RING * RING * 2)
    part = rows // PARTS
    group = 2 * RING * rows
    n_chunks = COLS // LANES
    dma = pltpu.SemaphoreType.DMA
    ring = lambda: [dma((n,)) for n in (SLOTS, ROUNDS, SLOTS, ROUNDS)]
    vmem = pl.BlockSpec(memory_space=pltpu.VMEM)
    return pl.pallas_call(
        kernel,
        out_shape=jax.ShapeDtypeStruct((rows, 2, COLS), F32),
        in_specs=[pl.BlockSpec(memory_space=pl.ANY)] * 4 + [pl.BlockSpec(memory_space=pltpu.SMEM)],
        out_specs=vmem,
        scratch_shapes=[
            pltpu.VMEM((1, nb), jnp.int32),
            pltpu.VMEM((1, nb), F32),
            pltpu.VMEM((1, coulomb.shape[0]), F32),
            pltpu.VMEM((ng, 4 * nb), BF16),
            pltpu.VMEM((2, 6 * nb, 2 * LANES), BF16),
            pltpu.VMEM((ng, LANES), F32),
            pltpu.VMEM((2, 1, LANES), F32),
            pltpu.VMEM((nb, LANES), F32),
            pltpu.VMEM((LANES, LANES), F32),
            pltpu.VMEM((STAGES, 2, nb, group), F32),
            pltpu.VMEM((n_chunks, 2, nb, LANES), F32),
            pltpu.VMEM((2, 2, 2, 2, 2, RING, part, LANES), F32),
            pltpu.VMEM((ROUNDS, 2, 2, 2, 2, RING, part, LANES), F32),
            pltpu.VMEM((SLOTS, 2, RING, 2, RING, part, LANES), F32),
            pltpu.VMEM((ROUNDS, 2, 2, RING, part, LANES), F32),
            pltpu.VMEM((ROUNDS, 2, 2, 2, RING, part, LANES), F32),
            pltpu.VMEM((SLOTS, 2, 2, RING, part, LANES), F32),
            pltpu.VMEM((ROUNDS, 2, RING, part, LANES), F32),
            pltpu.VMEM((SLOTS, 2, RING, part, LANES), F32),
            pltpu.VMEM((ROUNDS, 2, 2, part // 2, LANES), F32),
            pltpu.VMEM((ROUNDS, 2, 2, part, LANES), F32),
            dma((STAGES,)), dma((1,)), dma((1,)), dma((n_chunks,)),
            dma((2, 2)), dma((ROUNDS, 2)),
            *ring(), *ring(),
            dma((SLOTS, 3)), dma((ROUNDS, 3)), dma((3,)),
        ],
        compiler_params=pltpu.CompilerParams(
            collective_id=0, has_side_effects=True, vmem_limit_bytes=67043328
        ),
        name="remainder_sums",
    )(
        matrix_elements, band_index.reshape(1, nb), band_weight.reshape(1, nb),
        coulomb.reshape(1, -1), occupied,
    )


def body(matrix_elements, band_index, occupied, band_weight, coulomb):
    return sums_of(matrix_elements, band_index, band_weight, coulomb, occupied)


def solution(mesh):
    finer = Mesh(
        mesh.devices.reshape(4, 2, 4, 2, mesh.shape["ga"]),
        ("band_0", "band_1", "band_2", "band_3", "ga"),
    )
    in_specs = (P(None, BAND, "ga"), P(BAND), P(), P(BAND), P())
    out_specs = P(GA_BAND, None, None)
    return jax.shard_map(body, mesh=finer, in_specs=in_specs, out_specs=out_specs, check_vma=False)
```

```python
import functools
import math

import jax
import jax.numpy as jnp
from jax import lax
from jax.experimental import pallas as pl
from jax.experimental.pallas import tpu as pltpu
from jax.sharding import Mesh
from jax.sharding import PartitionSpec as P

COLS = 512
LANES = 128
BAND = ("band_0", "band_1", "band_2", "band_3")
GA_BAND = ("ga", "band_0", "band_1", "band_2", "band_3")
MESH = pl.DeviceIdType.MESH
Z_ORDER = (2, 3, 1, 0)
Z_GROUP = (0, 1, 1, 2)
RING = 4
PARTS = 2
ROUNDS = 4 * PARTS
LAGS = (2, 3, 4, 5)
SLOTS = 4
STAGES = 4
F32 = jnp.float32
BF16 = jnp.bfloat16


def split(x):
    hi = x.astype(BF16)
    return hi, (x - hi.astype(F32)).astype(BF16)


def kernel(
    m_ref, bi_in, bw_in, coul_in, occ_ref, o_ref,
    bi_ref, bw_ref, coul_ref, at, wst, rdef, cdef, coef, rowc, stage, slab, psend, pin,
    q, t1in, din, r1, zin, rz, t1in2, din2,
    stage_sem, slab_copy, slab_send, slab_recv, pair_send, pair_recv,
    t1_send, t1_recv, in_send, in_recv, t1_send2, t1_recv2, in_send2, in_recv2,
    z_send, z_recv, small_sem,
):
    rows = o_ref.shape[0]
    half = rows // 2
    part = rows // PARTS
    nb = m_ref.shape[1]
    ng = m_ref.shape[2]
    n_chunks = COLS // LANES
    scale = 1.0 / math.sqrt(nb * 2 * RING * RING * 2)
    group = 2 * RING * rows
    y, z, x, core, ga = (lax.axis_index(name) for name in ("band_0", "band_1", "band_2", "band_3", "ga"))
    up = lambda i: lax.rem(i + 1, RING)
    down = lambda i: lax.rem(i + RING - 1, RING)
    opposite = lambda i: lax.rem(i + 2, RING)

    barrier = pltpu.get_barrier_semaphore()
    peers = (
        {"ga": 1 - ga},
        {"band_2": up(x)},
        {"band_2": down(x)},
        {"band_0": up(y)},
        {"band_0": down(y)},
        {"band_1": 1 - z},
        {"band_3": 1 - core},
    )
    for peer in peers:
        pl.semaphore_signal(barrier, inc=1, device_id=peer, device_id_type=MESH)

    def stage_copy(i):
        start = pl.multiple_of(i * group, LANES)
        return pltpu.make_async_copy(
            m_ref.at[:, :, pl.ds(start, group)], stage.at[lax.rem(i, STAGES)], stage_sem.at[lax.rem(i, STAGES)]
        )

    def size_of(ref, send_sem, recv_sem):
        return pltpu.make_async_remote_copy(
            ref, ref, send_sem, recv_sem, device_id={"band_3": 1 - core}, device_id_type=MESH
        )

    def slab_local(j):
        return pltpu.make_async_copy(m_ref.at[:, :, pl.ds(j * LANES, LANES)], slab.at[j], slab_copy.at[0])

    def slab_remote(j):
        return pltpu.make_async_remote_copy(
            slab.at[j], slab.at[j], slab_send.at[0], slab_recv.at[j],
            device_id={"ga": 1 - ga}, device_id_type=MESH,
        )

    @pl.when(ga == 0)
    def _():
        for j in range(n_chunks):
            slab_local(j).start()

    small = [
        pltpu.make_async_copy(src, dst, small_sem.at[n])
        for n, (src, dst) in enumerate(((bi_in, bi_ref), (bw_in, bw_ref), (coul_in, coul_ref)))
    ]
    stage_copy(jnp.int32(0)).start()
    for copy in small:
        copy.start()
    for i in range(1, STAGES):
        stage_copy(jnp.int32(i)).start()
    for copy in small:
        copy.wait()

    c_row = (0.5 - (bi_ref[...] < occ_ref[0]).astype(F32)) * bw_ref[...]
    for i in range(nb // LANES):
        piece = c_row[:, i * LANES : (i + 1) * LANES]
        coef[pl.ds(i * LANES, LANES), :] = jnp.broadcast_to(piece, (LANES, LANES)).T

    @pl.when(ga == 0)
    def _():
        pltpu.make_async_copy(slab, slab, slab_copy.at[0]).wait()

    pl.semaphore_wait(barrier, len(peers))

    @pl.when(ga == 0)
    def _():
        for j in range(n_chunks):
            slab_remote(j).start()

    total_g = coul_ref.shape[1]
    row_start = ga * ng + (((y * 2 + z) * RING + x) * 2 + core) * rows
    block = (row_start // LANES) * LANES
    after = lax.rem(block + LANES, total_g)
    window = jnp.concatenate(
        [coul_ref[:, pl.ds(pl.multiple_of(b, LANES), LANES)] for b in (block, after)], 1
    )
    window = pltpu.roll(jnp.broadcast_to(window, (8, 2 * LANES)), lax.rem(2 * LANES - (row_start - block), 2 * LANES), 1)
    rowc[...] = jnp.broadcast_to(window[:1, :LANES], (LANES, LANES)).T

    def prep(i, carry):
        slot = lax.rem(i, STAGES)
        stage_copy(i).wait()

        def column(k, carry):
            lanes = pl.ds(pl.multiple_of(k * LANES, LANES), LANES)
            here = pl.ds(pl.multiple_of(i * group + k * LANES, LANES), LANES)
            a = stage[slot, 0, :, lanes]
            b = stage[slot, 1, :, lanes]
            a_hi, a_lo = split(a)
            b_hi, b_lo = split(b)
            at[here, 0:nb] = a_hi.T
            at[here, nb : 2 * nb] = b_hi.T
            at[here, 2 * nb : 3 * nb] = a_lo.T
            at[here, 3 * nb : 4 * nb] = b_lo.T
            share = 0.5 * jnp.sum(coef[...] * (2.0 - a * a - b * b), axis=0, keepdims=True)
            rdef[here, :] = jnp.broadcast_to(share, (LANES, LANES)).T
            return carry

        lax.fori_loop(0, group // LANES, column, 0, unroll=2)

        @pl.when(i + STAGES < 2 * RING)
        def _():
            stage_copy(i + STAGES).start()

        return carry

    lax.fori_loop(0, 2 + (2 * RING - 2) * ga, prep, 0)

    def weights(j):
        @pl.when(ga == 1)
        def _():
            slab_remote(j).wait_recv()

        w = lax.rem(j, 2)
        a = slab[j, 0]
        b = slab[j, 1]
        c = coef[...]
        cdef[w] = 0.5 * jnp.sum(c * (2.0 - a * a - b * b), axis=0, keepdims=True)
        a_hi, a_lo = split(c * a)
        b_hi, b_lo = split(c * b)
        for at_row, aa, bb in ((0, a_hi, b_hi), (2 * nb, a_hi, b_hi), (4 * nb, a_lo, b_lo)):
            wst[w, at_row : at_row + nb, 0:LANES] = aa
            wst[w, at_row : at_row + nb, LANES:] = bb
            wst[w, at_row + nb : at_row + 2 * nb, 0:LANES] = bb
            wst[w, at_row + nb : at_row + 2 * nb, LANES:] = -aa

    pieces = [(zd, xx) for zd in range(2) for xx in range(RING)]

    def product(r, g, parity):
        w = lax.rem(r // PARTS, 2)
        base = g * (2 * group) + parity * rows + lax.rem(r, PARTS) * part
        spots = [
            pl.ds(pl.multiple_of(base + zd * group + 2 * xx * rows, 16), part)
            for zd, xx in pieces
        ]
        left = jnp.concatenate([at[s, :] for s in spots], 0)
        left = jnp.concatenate([left, left[:, : 2 * nb]], 1)
        out = jnp.dot(left, wst[w], preferred_element_type=F32)
        shift = jnp.concatenate([rdef[s, :] for s in spots], 0) + cdef[w]
        return out[:, :LANES] + shift, out[:, LANES:]

    def pair_copy(r, g):
        return pltpu.make_async_remote_copy(
            psend.at[lax.rem(r, 2), g], pin.at[r, g], pair_send.at[lax.rem(r, 2), g], pair_recv.at[r, g],
            device_id={"band_3": 1 - core}, device_id_type=MESH,
        )

    def give(r):
        @pl.when(lax.rem(r, PARTS) == 0)
        def _():
            weights(r // PARTS)

        def one_pair(g, carry):
            @pl.when((r == 0) & (g > 0))
            def _():
                first = 2 * g * (1 - ga)
                lax.fori_loop(first, first + 2 * (1 - ga), prep, 0)

            @pl.when(r >= 2)
            def _():
                pair_copy(r - 2, g).wait_send()

            re, im = product(r, g, 1 - core)
            for n, (zd, xx) in enumerate(pieces):
                psend[lax.rem(r, 2), g, 0, zd, xx] = re[n * part : (n + 1) * part]
                psend[lax.rem(r, 2), g, 1, zd, xx] = im[n * part : (n + 1) * part]
            pair_copy(r, g).start()
            return carry

        lax.fori_loop(0, RING, one_pair, 0)

    def keep(r):
        slot = lax.rem(r, SLOTS)

        def one_pair(g, carry):
            re, im = product(r, g, core)
            pair_copy(r, g).wait_recv()
            for n, (zd, xx) in enumerate(pieces):
                q[slot, 0, xx, zd, g] = re[n * part : (n + 1) * part] + pin[r, g, 0, zd, xx]
                q[slot, 1, g, zd, xx] = im[n * part : (n + 1) * part] + pin[r, g, 1, zd, xx]
            return carry

        lax.fori_loop(0, RING, one_pair, 0)

    class Stage:
        def __init__(self, held, slots, tin, landed, cut, sems, axes):
            self.held, self.slots, self.tin, self.landed = held, slots, tin, landed
            self.cut, self.sems, self.axes = cut, sems, axes

        def send(self, which, r, k, way):
            name, me = self.axes[k]
            to = up(me) if way == 0 else down(me)
            here = self.cut(way if which != 1 else 1 - way)
            chunk = (lax.rem(r, self.slots), k, opposite(me) if which == 0 else to)
            src = self.held.at[chunk + here]
            dst = self.tin.at[r, k, way] if which == 0 else self.landed.at[(r, k, way) + here]
            ss, rs = self.sems[min(which, 1)]
            return pltpu.make_async_remote_copy(
                src, dst, ss.at[lax.rem(r, self.slots)], rs.at[r], device_id={name: to}, device_id_type=MESH
            )

        def whole(self, which, r):
            ref = (self.tin if which == 0 else self.landed).at[r]
            ss, rs = self.sems[which]
            return size_of(ref, ss.at[lax.rem(r, self.slots)], rs.at[r])

        def begin(self, r, which, k):
            for way in range(2):
                self.send(which, r, k, way).start()

        def combine(self, r):
            self.whole(0, r).wait_recv()
            for k in range(2):
                me = self.axes[k][1]
                for way in range(2):
                    to = up(me) if way == 0 else down(me)
                    here = (lax.rem(r, self.slots), k, to) + self.cut(way)
                    self.held[here] += self.tin[r, k, way]
                    self.send(2, r, k, way).start()

        def arrived(self, r):
            self.whole(1, r).wait_recv()

        def total(self, r, k):
            return self.held[lax.rem(r, self.slots), k, self.axes[k][1]] + self.landed[r, k, 0] + self.landed[r, k, 1]

        def sent(self, r):
            self.whole(0, r).wait_send()
            self.whole(1, r).wait_send()

    along_x, along_y = ("band_2", x), ("band_0", y)
    one = Stage(
        q, SLOTS, t1in, din, lambda h: (h,),
        ((t1_send, t1_recv), (in_send, in_recv)), (along_x, along_y),
    )
    two = Stage(
        rz, 2, t1in2, din2, lambda h: (pl.ds(h * half, half),),
        ((t1_send2, t1_recv2), (in_send2, in_recv2)), (along_y, along_x),
    )

    def z_copy(r, k, m):
        e = lax.rem(two.axes[k][1] + Z_ORDER[m], RING)
        return pltpu.make_async_remote_copy(
            r1.at[lax.rem(r, SLOTS), k, 1 - z, e], zin.at[r, k, e],
            z_send.at[lax.rem(r, SLOTS), Z_GROUP[m]], z_recv.at[r, Z_GROUP[m]],
            device_id={"band_1": 1 - z}, device_id_type=MESH,
        )

    def z_whole(r, n):
        ref = zin.at[r, :, pl.ds(n, Z_GROUP.count(n))]
        return size_of(ref, z_send.at[lax.rem(r, SLOTS), n], z_recv.at[r, n])

    def to_other_z(t):
        one.arrived(t)
        for k in range(2):
            r1[lax.rem(t, SLOTS), k] = one.total(t, k)
        for m in range(RING):
            for k in range(2):
                z_copy(t, k, m).start()

    def sub_rows(t):
        return pl.ds(pl.multiple_of(lax.rem(t, PARTS) * part, 8), part)

    def join(t, k, m):
        e = lax.rem(two.axes[k][1] + Z_ORDER[m], RING)
        here = (lax.rem(t // PARTS, 2), k, e, sub_rows(t), slice(None))
        rz[here] = r1[lax.rem(t, SLOTS), k, z, e] + zin[t, k, e]

    def from_other_z(t):
        last = lax.rem(t, PARTS) == PARTS - 1
        for which in range(2):
            z_whole(t, which).wait_recv()
            for k in range(2):
                for m in (m for m in range(RING) if Z_GROUP[m] == which):
                    join(t, k, m)

            @pl.when(last)
            def _():
                for k in range(2):
                    two.begin(t // PARTS, which, k)

        z_whole_last(t, lax.rem(t, PARTS) < PARTS - 1)
        one.sent(t)

    def z_whole_last(t, now):
        @pl.when(now)
        def _():
            z_whole(t, 2).wait_recv()
            for k in range(2):
                join(t, k, RING - 1)

    def second_combine(t):
        @pl.when(lax.rem(t, PARTS) == PARTS - 1)
        def _():
            two.combine(t // PARTS)

        for n in range(3):
            z_whole(t, n).wait_send()

    def finish(t):
        z_whole_last(t, lax.rem(t, PARTS) == PARTS - 1)

        @pl.when(lax.rem(t, PARTS) == PARTS - 1)
        def _():
            j = t // PARTS
            lanes = pl.ds(pl.multiple_of(j * LANES, LANES), LANES)
            weight = jnp.sqrt(rowc[0:rows, :] * coul_ref[:, lanes]) * scale
            two.arrived(j)
            for k in range(2):
                o_ref[:, k, lanes] = two.total(j, k) * weight
            two.sent(j)

    def step(r, carry):
        @pl.when((r >= 0) & (r < ROUNDS))
        def _():
            keep(r)
            for k in range(2):
                one.begin(r, 0, k)

        @pl.when((r >= 1) & (r < ROUNDS + 1))
        def _():
            one.combine(r - 1)

        @pl.when((r >= 0) & (r < ROUNDS))
        def _():
            for k in range(2):
                one.begin(r, 1, k)

        @pl.when(r + 1 < ROUNDS)
        def _():
            give(r + 1)

        def late(lag, stage_work):
            @pl.when((r >= lag) & (r < ROUNDS + lag))
            def _():
                stage_work(r - lag)

        for lag, stage_work in zip(LAGS, (to_other_z, from_other_z, second_combine, finish)):
            late(lag, stage_work)

        return carry

    lax.fori_loop(-1, ROUNDS + LAGS[-1], step, 0)

    for g in range(RING):
        pair_copy(ROUNDS - 2, g).wait_send()
        pair_copy(ROUNDS - 1, g).wait_send()

    @pl.when(ga == 0)
    def _():
        size_of(slab, slab_send.at[0], slab_recv.at[0]).wait_send()


def sums_of(matrix_elements, band_index, band_weight, coulomb, occupied):
    nb, ng = matrix_elements.shape[1:]
    rows = ng // (2 * RING * RING * 2)
    part = rows // PARTS
    group = 2 * RING * rows
    n_chunks = COLS // LANES
    dma = pltpu.SemaphoreType.DMA
    ring = lambda slots, n: [dma((slots,)), dma((n,)), dma((slots,)), dma((n,))]
    vmem = pl.BlockSpec(memory_space=pltpu.VMEM)
    return pl.pallas_call(
        kernel,
        out_shape=jax.ShapeDtypeStruct((rows, 2, COLS), F32),
        in_specs=[pl.BlockSpec(memory_space=pl.ANY)] * 4 + [pl.BlockSpec(memory_space=pltpu.SMEM)],
        out_specs=vmem,
        scratch_shapes=[
            pltpu.VMEM((1, nb), jnp.int32),
            pltpu.VMEM((1, nb), F32),
            pltpu.VMEM((1, coulomb.shape[0]), F32),
            pltpu.VMEM((ng, 4 * nb), BF16),
            pltpu.VMEM((2, 6 * nb, 2 * LANES), BF16),
            pltpu.VMEM((ng, LANES), F32),
            pltpu.VMEM((2, 1, LANES), F32),
            pltpu.VMEM((nb, LANES), F32),
            pltpu.VMEM((LANES, LANES), F32),
            pltpu.VMEM((STAGES, 2, nb, group), F32),
            pltpu.VMEM((n_chunks, 2, nb, LANES), F32),
            pltpu.VMEM((2, RING, 2, 2, RING, part, LANES), F32),
            pltpu.VMEM((ROUNDS, RING, 2, 2, RING, part, LANES), F32),
            pltpu.VMEM((SLOTS, 2, RING, 2, RING, part, LANES), F32),
            pltpu.VMEM((ROUNDS, 2, 2, RING, part, LANES), F32),
            pltpu.VMEM((ROUNDS, 2, 2, 2, RING, part, LANES), F32),
            pltpu.VMEM((SLOTS, 2, 2, RING, part, LANES), F32),
            pltpu.VMEM((ROUNDS, 2, RING, part, LANES), F32),
            pltpu.VMEM((2, 2, RING, rows, LANES), F32),
            pltpu.VMEM((n_chunks, 2, 2, rows // 2, LANES), F32),
            pltpu.VMEM((n_chunks, 2, 2, rows, LANES), F32),
            dma((STAGES,)), dma((1,)), dma((1,)), dma((n_chunks,)),
            dma((2, RING)), dma((ROUNDS, RING)),
            *ring(SLOTS, ROUNDS), *ring(2, n_chunks),
            dma((SLOTS, 3)), dma((ROUNDS, 3)), dma((3,)),
        ],
        compiler_params=pltpu.CompilerParams(
            collective_id=0, has_side_effects=True, vmem_limit_bytes=67043328
        ),
        name="remainder_sums",
    )(
        matrix_elements, band_index.reshape(1, nb), band_weight.reshape(1, nb),
        coulomb.reshape(1, -1), occupied,
    )


def body(matrix_elements, band_index, occupied, band_weight, coulomb):
    return sums_of(matrix_elements, band_index, band_weight, coulomb, occupied)


def solution(mesh):
    finer = Mesh(
        mesh.devices.reshape(4, 2, 4, 2, mesh.shape["ga"]),
        ("band_0", "band_1", "band_2", "band_3", "ga"),
    )
    in_specs = (P(None, BAND, "ga"), P(BAND), P(), P(BAND), P())
    out_specs = P(GA_BAND, None, None)
    return jax.shard_map(body, mesh=finer, in_specs=in_specs, out_specs=out_specs, check_vma=False)
```

```python
import functools
import math

import jax
import jax.numpy as jnp
from jax import lax
from jax.experimental import pallas as pl
from jax.experimental.pallas import tpu as pltpu
from jax.sharding import Mesh
from jax.sharding import PartitionSpec as P

COLS = 512
LANES = 128
BAND = ("band_0", "band_1", "band_2", "band_3")
GA_BAND = ("ga", "band_0", "band_1", "band_2", "band_3")
MESH = pl.DeviceIdType.MESH
Z_ORDER = (2, 3, 1, 0)
Z_GROUP = (0, 1, 1, 2)
RING = 4
PARTS = 2
ROUNDS = 4 * PARTS
LAGS = (2, 3, 4, 5)
SLOTS = 4
STAGES = 4
F32 = jnp.float32
BF16 = jnp.bfloat16


def split(x):
    hi = x.astype(BF16)
    return hi, (x - hi.astype(F32)).astype(BF16)


def kernel(
    m_ref, bi_in, bw_in, coul_in, occ_ref, o_ref,
    bi_ref, bw_ref, coul_ref, at, wst, rdef, cdef, coef, rowc, stage, slab, psend, pin,
    q, t1in, din, r1, zin, rz, t1in2, din2,
    stage_sem, slab_copy, slab_send, slab_recv, pair_send, pair_recv,
    t1_send, t1_recv, in_send, in_recv, t1_send2, t1_recv2, in_send2, in_recv2,
    z_send, z_recv, small_sem,
):
    rows = o_ref.shape[0]
    half = rows // 2
    part = rows // PARTS
    nb = m_ref.shape[1]
    ng = m_ref.shape[2]
    n_chunks = COLS // LANES
    scale = 1.0 / math.sqrt(nb * 2 * RING * RING * 2)
    group = 2 * RING * rows
    y, z, x, core, ga = (lax.axis_index(name) for name in ("band_0", "band_1", "band_2", "band_3", "ga"))
    up = lambda i: lax.rem(i + 1, RING)
    down = lambda i: lax.rem(i + RING - 1, RING)
    opposite = lambda i: lax.rem(i + 2, RING)

    barrier = pltpu.get_barrier_semaphore()
    peers = (
        {"ga": 1 - ga},
        {"band_2": up(x)},
        {"band_2": down(x)},
        {"band_0": up(y)},
        {"band_0": down(y)},
        {"band_1": 1 - z},
        {"band_3": 1 - core},
    )
    for peer in peers:
        pl.semaphore_signal(barrier, inc=1, device_id=peer, device_id_type=MESH)

    def stage_copy(i):
        start = pl.multiple_of(i * group, LANES)
        return pltpu.make_async_copy(
            m_ref.at[:, :, pl.ds(start, group)], stage.at[lax.rem(i, STAGES)], stage_sem.at[lax.rem(i, STAGES)]
        )

    def size_of(ref, send_sem, recv_sem):
        return pltpu.make_async_remote_copy(
            ref, ref, send_sem, recv_sem, device_id={"band_3": 1 - core}, device_id_type=MESH
        )

    def slab_local(j):
        return pltpu.make_async_copy(m_ref.at[:, :, pl.ds(j * LANES, LANES)], slab.at[j], slab_copy.at[min(j, 1)])

    def slab_remote(j):
        return pltpu.make_async_remote_copy(
            slab.at[j], slab.at[j], slab_send.at[0], slab_recv.at[j],
            device_id={"ga": 1 - ga}, device_id_type=MESH,
        )

    @pl.when(ga == 0)
    def _():
        slab_local(0).start()

    small = [
        pltpu.make_async_copy(src, dst, small_sem.at[n])
        for n, (src, dst) in enumerate(((bi_in, bi_ref), (bw_in, bw_ref), (coul_in, coul_ref)))
    ]
    stage_copy(jnp.int32(0)).start()
    for copy in small:
        copy.start()
    for i in range(1, STAGES):
        stage_copy(jnp.int32(i)).start()
    @pl.when(ga == 0)
    def _():
        for j in range(1, n_chunks):
            slab_local(j).start()

    @pl.when(ga == 0)
    def _():
        slab_local(0).wait()

    pl.semaphore_wait(barrier, len(peers))

    @pl.when(ga == 0)
    def _():
        slab_remote(0).start()
        rest = slab.at[pl.ds(1, n_chunks - 1)]
        pltpu.make_async_copy(rest, rest, slab_copy.at[1]).wait()
        for j in range(1, n_chunks):
            slab_remote(j).start()

    for copy in small:
        copy.wait()

    c_row = (0.5 - (bi_ref[...] < occ_ref[0]).astype(F32)) * bw_ref[...]
    for i in range(nb // LANES):
        piece = c_row[:, i * LANES : (i + 1) * LANES]
        coef[pl.ds(i * LANES, LANES), :] = jnp.broadcast_to(piece, (LANES, LANES)).T

    total_g = coul_ref.shape[1]
    row_start = ga * ng + (((y * 2 + z) * RING + x) * 2 + core) * rows
    block = (row_start // LANES) * LANES
    after = lax.rem(block + LANES, total_g)
    window = jnp.concatenate(
        [coul_ref[:, pl.ds(pl.multiple_of(b, LANES), LANES)] for b in (block, after)], 1
    )
    window = pltpu.roll(jnp.broadcast_to(window, (8, 2 * LANES)), lax.rem(2 * LANES - (row_start - block), 2 * LANES), 1)
    rowc[...] = jnp.broadcast_to(window[:1, :LANES], (LANES, LANES)).T

    def prep(i, carry):
        slot = lax.rem(i, STAGES)
        stage_copy(i).wait()

        def column(k, carry):
            lanes = pl.ds(pl.multiple_of(k * LANES, LANES), LANES)
            here = pl.ds(pl.multiple_of(i * group + k * LANES, LANES), LANES)
            a = stage[slot, 0, :, lanes]
            b = stage[slot, 1, :, lanes]
            a_hi, a_lo = split(a)
            b_hi, b_lo = split(b)
            at[here, 0:nb] = a_hi.T
            at[here, nb : 2 * nb] = b_hi.T
            at[here, 2 * nb : 3 * nb] = a_lo.T
            at[here, 3 * nb : 4 * nb] = b_lo.T
            share = 0.5 * jnp.sum(coef[...] * (2.0 - a * a - b * b), axis=0, keepdims=True)
            rdef[here, :] = jnp.broadcast_to(share, (LANES, LANES)).T
            return carry

        lax.fori_loop(0, group // LANES, column, 0, unroll=2)

        @pl.when(i + STAGES < 2 * RING)
        def _():
            stage_copy(i + STAGES).start()

        return carry

    lax.fori_loop(0, 2 + (2 * RING - 2) * ga, prep, 0)

    def weights(j):
        @pl.when(ga == 1)
        def _():
            slab_remote(j).wait_recv()

        w = lax.rem(j, 2)
        a = slab[j, 0]
        b = slab[j, 1]
        c = coef[...]
        cdef[w] = 0.5 * jnp.sum(c * (2.0 - a * a - b * b), axis=0, keepdims=True)
        a_hi, a_lo = split(c * a)
        b_hi, b_lo = split(c * b)
        for at_row, aa, bb in ((0, a_hi, b_hi), (2 * nb, a_hi, b_hi), (4 * nb, a_lo, b_lo)):
            wst[w, at_row : at_row + nb, 0:LANES] = aa
            wst[w, at_row : at_row + nb, LANES:] = bb
            wst[w, at_row + nb : at_row + 2 * nb, 0:LANES] = bb
            wst[w, at_row + nb : at_row + 2 * nb, LANES:] = -aa

    pieces = [(zd, xx) for zd in range(2) for xx in range(RING)]

    def product(r, g, parity):
        w = lax.rem(r // PARTS, 2)
        base = g * (2 * group) + parity * rows + lax.rem(r, PARTS) * part
        spots = [
            pl.ds(pl.multiple_of(base + zd * group + 2 * xx * rows, 16), part)
            for zd, xx in pieces
        ]
        left = jnp.concatenate([at[s, :] for s in spots], 0)
        left = jnp.concatenate([left, left[:, : 2 * nb]], 1)
        out = jnp.dot(left, wst[w], preferred_element_type=F32)
        shift = jnp.concatenate([rdef[s, :] for s in spots], 0) + cdef[w]
        return out[:, :LANES] + shift, out[:, LANES:]

    def pair_copy(r, g):
        return pltpu.make_async_remote_copy(
            psend.at[lax.rem(r, 2), g], pin.at[lax.rem(r, 2), g], pair_send.at[lax.rem(r, 2), g], pair_recv.at[lax.rem(r, 2), g],
            device_id={"band_3": 1 - core}, device_id_type=MESH,
        )

    def give(r):
        @pl.when(lax.rem(r, PARTS) == 0)
        def _():
            weights(r // PARTS)

        def one_pair(g, carry):
            @pl.when((r == 0) & (g > 0))
            def _():
                first = 2 * g * (1 - ga)
                lax.fori_loop(first, first + 2 * (1 - ga), prep, 0)

            @pl.when(r >= 2)
            def _():
                pair_copy(r - 2, g).wait_send()

            re, im = product(r, g, 1 - core)
            for n, (zd, xx) in enumerate(pieces):
                psend[lax.rem(r, 2), g, 0, zd, xx] = re[n * part : (n + 1) * part]
                psend[lax.rem(r, 2), g, 1, zd, xx] = im[n * part : (n + 1) * part]
            pair_copy(r, g).start()
            return carry

        lax.fori_loop(0, RING, one_pair, 0)

    def keep(r):
        slot = lax.rem(r, SLOTS)

        def one_pair(g, carry):
            re, im = product(r, g, core)
            pair_copy(r, g).wait_recv()
            for n, (zd, xx) in enumerate(pieces):
                q[slot, 0, xx, zd, g] = re[n * part : (n + 1) * part] + pin[lax.rem(r, 2), g, 0, zd, xx]
                q[slot, 1, g, zd, xx] = im[n * part : (n + 1) * part] + pin[lax.rem(r, 2), g, 1, zd, xx]
            return carry

        lax.fori_loop(0, RING, one_pair, 0)

    class Stage:
        def __init__(self, held, slots, tin, landed, cut, sems, axes):
            self.held, self.slots, self.tin, self.landed = held, slots, tin, landed
            self.cut, self.sems, self.axes = cut, sems, axes

        def send(self, which, r, k, way):
            name, me = self.axes[k]
            to = up(me) if way == 0 else down(me)
            here = self.cut(way if which != 1 else 1 - way)
            chunk = (lax.rem(r, self.slots), k, opposite(me) if which == 0 else to)
            src = self.held.at[chunk + here]
            dst = self.tin.at[r, k, way] if which == 0 else self.landed.at[(r, k, way) + here]
            ss, rs = self.sems[min(which, 1)]
            return pltpu.make_async_remote_copy(
                src, dst, ss.at[lax.rem(r, self.slots)], rs.at[r], device_id={name: to}, device_id_type=MESH
            )

        def whole(self, which, r):
            ref = (self.tin if which == 0 else self.landed).at[r]
            ss, rs = self.sems[which]
            return size_of(ref, ss.at[lax.rem(r, self.slots)], rs.at[r])

        def begin(self, r, which, k):
            for way in range(2):
                self.send(which, r, k, way).start()

        def combine(self, r):
            self.whole(0, r).wait_recv()
            for k in range(2):
                me = self.axes[k][1]
                for way in range(2):
                    to = up(me) if way == 0 else down(me)
                    here = (lax.rem(r, self.slots), k, to) + self.cut(way)
                    self.held[here] += self.tin[r, k, way]
                    self.send(2, r, k, way).start()

        def arrived(self, r):
            self.whole(1, r).wait_recv()

        def total(self, r, k):
            return self.held[lax.rem(r, self.slots), k, self.axes[k][1]] + self.landed[r, k, 0] + self.landed[r, k, 1]

        def sent(self, r):
            self.whole(0, r).wait_send()
            self.whole(1, r).wait_send()

    along_x, along_y = ("band_2", x), ("band_0", y)
    one = Stage(
        q, SLOTS, t1in, din, lambda h: (h,),
        ((t1_send, t1_recv), (in_send, in_recv)), (along_x, along_y),
    )
    two = Stage(
        rz, 2, t1in2, din2, lambda h: (pl.ds(h * half, half),),
        ((t1_send2, t1_recv2), (in_send2, in_recv2)), (along_y, along_x),
    )

    def z_copy(r, k, m):
        e = lax.rem(two.axes[k][1] + Z_ORDER[m], RING)
        return pltpu.make_async_remote_copy(
            r1.at[lax.rem(r, SLOTS), k, 1 - z, e], zin.at[r, k, e],
            z_send.at[lax.rem(r, SLOTS), Z_GROUP[m]], z_recv.at[r, Z_GROUP[m]],
            device_id={"band_1": 1 - z}, device_id_type=MESH,
        )

    def z_whole(r, n):
        ref = zin.at[r, :, pl.ds(n, Z_GROUP.count(n))]
        return size_of(ref, z_send.at[lax.rem(r, SLOTS), n], z_recv.at[r, n])

    def to_other_z(t):
        one.arrived(t)
        for k in range(2):
            r1[lax.rem(t, SLOTS), k] = one.total(t, k)
        for m in range(RING):
            for k in range(2):
                z_copy(t, k, m).start()

    def sub_rows(t):
        return pl.ds(pl.multiple_of(lax.rem(t, PARTS) * part, 8), part)

    def join(t, k, m):
        e = lax.rem(two.axes[k][1] + Z_ORDER[m], RING)
        here = (lax.rem(t // PARTS, 2), k, e, sub_rows(t), slice(None))
        rz[here] = r1[lax.rem(t, SLOTS), k, z, e] + zin[t, k, e]

    def from_other_z(t):
        last = lax.rem(t, PARTS) == PARTS - 1
        for which in range(2):
            z_whole(t, which).wait_recv()
            for k in range(2):
                for m in (m for m in range(RING) if Z_GROUP[m] == which):
                    join(t, k, m)

            @pl.when(last)
            def _():
                for k in range(2):
                    two.begin(t // PARTS, which, k)

        z_whole_last(t, lax.rem(t, PARTS) < PARTS - 1)
        one.sent(t)

    def z_whole_last(t, now):
        @pl.when(now)
        def _():
            z_whole(t, 2).wait_recv()
            for k in range(2):
                join(t, k, RING - 1)

    def second_combine(t):
        @pl.when(lax.rem(t, PARTS) == PARTS - 1)
        def _():
            two.combine(t // PARTS)

        for n in range(3):
            z_whole(t, n).wait_send()

    def finish(t):
        z_whole_last(t, lax.rem(t, PARTS) == PARTS - 1)

        @pl.when(lax.rem(t, PARTS) == PARTS - 1)
        def _():
            j = t // PARTS
            lanes = pl.ds(pl.multiple_of(j * LANES, LANES), LANES)
            weight = jnp.sqrt(rowc[0:rows, :] * coul_ref[:, lanes]) * scale
            two.arrived(j)
            for k in range(2):
                o_ref[:, k, lanes] = two.total(j, k) * weight
            two.sent(j)

    def step(r, carry):
        @pl.when((r >= 0) & (r < ROUNDS))
        def _():
            keep(r)
            for k in range(2):
                one.begin(r, 0, k)

        @pl.when(r + 1 < ROUNDS)
        def _():
            give(r + 1)

        @pl.when((r >= 1) & (r < ROUNDS + 1))
        def _():
            one.combine(r - 1)

        @pl.when((r >= 0) & (r < ROUNDS))
        def _():
            for k in range(2):
                one.begin(r, 1, k)

        def late(lag, stage_work):
            @pl.when((r >= lag) & (r < ROUNDS + lag))
            def _():
                stage_work(r - lag)

        for lag, stage_work in zip(LAGS, (to_other_z, from_other_z, second_combine, finish)):
            late(lag, stage_work)

        return carry

    lax.fori_loop(-1, ROUNDS + LAGS[-1], step, 0)

    for g in range(RING):
        pair_copy(ROUNDS - 2, g).wait_send()
        pair_copy(ROUNDS - 1, g).wait_send()

    @pl.when(ga == 0)
    def _():
        size_of(slab, slab_send.at[0], slab_recv.at[0]).wait_send()


def sums_of(matrix_elements, band_index, band_weight, coulomb, occupied):
    nb, ng = matrix_elements.shape[1:]
    rows = ng // (2 * RING * RING * 2)
    part = rows // PARTS
    group = 2 * RING * rows
    n_chunks = COLS // LANES
    dma = pltpu.SemaphoreType.DMA
    ring = lambda slots, n: [dma((slots,)), dma((n,)), dma((slots,)), dma((n,))]
    vmem = pl.BlockSpec(memory_space=pltpu.VMEM)
    return pl.pallas_call(
        kernel,
        out_shape=jax.ShapeDtypeStruct((rows, 2, COLS), F32),
        in_specs=[pl.BlockSpec(memory_space=pl.ANY)] * 4 + [pl.BlockSpec(memory_space=pltpu.SMEM)],
        out_specs=vmem,
        scratch_shapes=[
            pltpu.VMEM((1, nb), jnp.int32),
            pltpu.VMEM((1, nb), F32),
            pltpu.VMEM((1, coulomb.shape[0]), F32),
            pltpu.VMEM((ng, 4 * nb), BF16),
            pltpu.VMEM((2, 6 * nb, 2 * LANES), BF16),
            pltpu.VMEM((ng, LANES), F32),
            pltpu.VMEM((2, 1, LANES), F32),
            pltpu.VMEM((nb, LANES), F32),
            pltpu.VMEM((LANES, LANES), F32),
            pltpu.VMEM((STAGES, 2, nb, group), F32),
            pltpu.VMEM((n_chunks, 2, nb, LANES), F32),
            pltpu.VMEM((2, RING, 2, 2, RING, part, LANES), F32),
            pltpu.VMEM((2, RING, 2, 2, RING, part, LANES), F32),
            pltpu.VMEM((SLOTS, 2, RING, 2, RING, part, LANES), F32),
            pltpu.VMEM((ROUNDS, 2, 2, RING, part, LANES), F32),
            pltpu.VMEM((ROUNDS, 2, 2, 2, RING, part, LANES), F32),
            pltpu.VMEM((SLOTS, 2, 2, RING, part, LANES), F32),
            pltpu.VMEM((ROUNDS, 2, RING, part, LANES), F32),
            pltpu.VMEM((2, 2, RING, rows, LANES), F32),
            pltpu.VMEM((n_chunks, 2, 2, rows // 2, LANES), F32),
            pltpu.VMEM((n_chunks, 2, 2, rows, LANES), F32),
            dma((STAGES,)), dma((2,)), dma((1,)), dma((n_chunks,)),
            dma((2, RING)), dma((2, RING)),
            *ring(SLOTS, ROUNDS), *ring(2, n_chunks),
            dma((SLOTS, 3)), dma((ROUNDS, 3)), dma((3,)),
        ],
        compiler_params=pltpu.CompilerParams(
            collective_id=0, has_side_effects=True, vmem_limit_bytes=54*1024*1024
        ),
        name="remainder_sums",
    )(
        matrix_elements, band_index.reshape(1, nb), band_weight.reshape(1, nb),
        coulomb.reshape(1, -1), occupied,
    )


def body(matrix_elements, band_index, occupied, band_weight, coulomb):
    return sums_of(matrix_elements, band_index, band_weight, coulomb, occupied)


def solution(mesh):
    finer = Mesh(
        mesh.devices.reshape(4, 2, 4, 2, mesh.shape["ga"]),
        ("band_0", "band_1", "band_2", "band_3", "ga"),
    )
    in_specs = (P(None, BAND, "ga"), P(BAND), P(), P(BAND), P())
    out_specs = P(GA_BAND, None, None)
    return jax.shard_map(body, mesh=finer, in_specs=in_specs, out_specs=out_specs, check_vma=False)
```
